32 devices in a mesh: mod: 2 (over y), exp: 16 (over z, x, core).
Axes of the slice: x: 2, y: 2, z: 4, core: 2. Of those that a mesh axis runs over, the one named last changes fastest.
Arguments:
- tokens: bfloat16 [2, 8192, 1024], P('mod', 'exp'), may hold values from -60 to 60
- bottleneck: bfloat16 [64, 4, 1024], P('exp'), may hold values from -6 to 6
- clip_ids: int32 [2, 8192], P('mod', 'exp'), may hold values from 0 to 63, as said below
- expert_ids: int32 [2, 8192], P('mod', 'exp'), may hold values from 0 to 15, as said below
- slots: int32 [2, 8192], P('mod', 'exp'), may hold values from 0 to 127, as said below
- norm1_gain: bfloat16 [2, 1024], P('mod'), may hold values from 0.099609375 to 1.8984375
- attn_qkv: bfloat16 [2, 1024, 3072], P('mod'), may hold values from -2 to 2
- attn_out: bfloat16 [2, 1024, 1024], P('mod'), may hold values from -0.1875 to 0.1875
- norm2_gain: bfloat16 [2, 1024], P('mod'), may hold values from 0.099609375 to 1.8984375
- router: bfloat16 [1024, 16], replicated, may hold values from -0.1875 to 0.1875
- fc_in: bfloat16 [16, 1024, 4096], P('exp'), may hold values from -0.1875 to 0.1875
- fc_out: bfloat16 [16, 4096, 1024], P('exp'), may hold values from -0.09375 to 0.09375
Outputs:
- mixed_tokens: bfloat16 [2, 8192, 1024], P('mod', 'exp')
- new_bottleneck: bfloat16 [64, 4, 1024], P('exp')
The draws below stay inside these ranges and needn't reach their ends.
Inputs may be any that keep to these rules, and one draw needn't show every extreme that they name: `clip_ids`: Non-decreasing in each modality; the tokens of block b of 512 rows belong to clips b * 4 to (b + 1) * 4 - 1, each of which has one or more of them. `expert_ids`: each token's single expert. For the k tokens of one block of 512 rows of one modality that share an expert, the slots are 0 to k - 1 in some order; k is at most 128; in every block of each modality one expert, the same for all blocks of that modality, has k = 128.
All inputs are finite; a program needn't handle non-finite values.
Results may differ from the reference program's by a relative error of at most 0.0085.
Values may be sent and summed in bfloat16 or wider, within the bound.
No kernel may reach another device: no remote copies, remote signals or barrier semaphores. Data moves between devices by JAX's collectives and lax.ppermute only.
A program may use at most 128 MiB of HBM per device.

```python
import math
import jax
import jax.numpy as jnp
from jax import lax

D = 1024
FF = 4096
HEAD = 64
NB = 4
TOK_DEV = 512
CLIPS_DEV = 4
EXPERTS = 16
TOKENS = 8192
CLIPS = 64
CAP = 64


def routing_table(key):
    blocks = TOKENS // TOK_DEV
    queue_len = 2 * CAP
    seat_count = EXPERTS * queue_len
    routing_key = jax.random.fold_in(key, 7001)
    hot_key, level_key, block_key = jax.random.split(routing_key, 3)
    hottest = jax.random.randint(hot_key, (2,), 0, EXPERTS)
    levels = jax.random.randint(level_key, (2, EXPERTS), 0, 4)
    block_seeds = jax.random.split(block_key, 2 * blocks)
    modality_of = jnp.arange(2 * blocks, dtype=jnp.int32) // blocks
    seat_index = jnp.arange(seat_count, dtype=jnp.int32)
    seat_expert = seat_index // queue_len

    def one_block(block_seed, modality):
        second_key, noise_key, order_key = jax.random.split(block_seed, 3)
        second = jax.random.randint(second_key, (), 0, EXPERTS)
        jitter = jax.random.randint(noise_key, (seat_count,), 0, 4096)
        favoured = (seat_expert == hottest[modality]) | (seat_expert == second)
        seat_score = jitter + levels[modality][seat_expert] * 1024 + jnp.where(favoured, 16384, 0)
        ranked = seat_score * seat_count + seat_index
        picked = lax.top_k(ranked, TOK_DEV)[1]
        marked = jnp.zeros((seat_count,), jnp.int32).at[picked].set(1)
        grouped = marked.reshape(EXPERTS, queue_len)
        rank_table = (jnp.cumsum(grouped, axis=1) - grouped).reshape(seat_count)
        token_order = jax.random.permutation(order_key, TOK_DEV)
        assigned = picked[token_order]
        return (seat_expert[assigned], rank_table[assigned])
    experts_drawn, slots_drawn = jax.vmap(one_block)(block_seeds, modality_of)
    return (experts_drawn.reshape(2, TOKENS).astype(jnp.int32), slots_drawn.reshape(2, TOKENS).astype(jnp.int32))


def draw_expert_ids(key, part):
    return routing_table(key)[0]


def draw_slots(key, part):
    return routing_table(key)[1]


def draw_clip_ids(key, part):
    blocks = TOKENS // TOK_DEV
    block_seeds = jax.random.split(jax.random.fold_in(key, 7002), 2 * blocks)
    position = jnp.arange(TOK_DEV, dtype=jnp.int32)

    def one_block(block_seed):
        cuts = jax.random.permutation(block_seed, TOK_DEV - 1)[:CLIPS_DEV - 1] + 1
        return jnp.sum((position[:, None] >= cuts[None, :]).astype(jnp.int32), axis=1)
    local_ids = jax.vmap(one_block)(block_seeds).reshape(2, blocks, TOK_DEV)
    offsets = jnp.arange(blocks, dtype=jnp.int32)[None, :, None] * CLIPS_DEV
    return (local_ids + offsets).reshape(2, TOKENS).astype(jnp.int32)


def draw_tokens(key, part):
    normal_draw = jnp.clip(jax.random.normal(key, (2, TOKENS, D), jnp.float32), -6.0, 6.0)
    return normal_draw.astype(jnp.bfloat16)


def draw_attn_qkv(key, part):
    unit_scale = 1.0 / math.sqrt(D)
    entries = jax.random.normal(key, (2, D, 3 * D), jnp.float32) * unit_scale
    return jnp.clip(entries, -2.0, 2.0).astype(jnp.bfloat16)


def shard_levels(stream_key, shape, pieces, smallest, top_value):
    gain = 1.0
    for dim, parts in pieces:
        steps = jax.random.uniform(jax.random.fold_in(jax.random.fold_in(stream_key, 6), dim), (parts,), jnp.float32, smallest / len(pieces), top_value / len(pieces))
        gain = gain * jnp.repeat(jnp.exp(steps), shape[dim] // parts).reshape((-1,) + (1,) * (len(shape) - 1 - dim))
    return gain


def scatter_about(stream_key, shape, scale, limit, cuts=(), kind=jnp.bfloat16):
    factor_of = shard_levels(stream_key, shape, cuts, -0.22, 0.18) if cuts else 1.0
    values = jax.random.normal(stream_key, shape, jnp.float32) * scale * factor_of
    return jnp.minimum(jnp.maximum(values, -limit), limit).astype(kind)


def setup_inputs(seed: int = 0) -> dict:
    key_list = jax.random.split(jax.random.key(seed), 13)
    return {
        "tokens": draw_tokens(jax.random.fold_in(key_list[12], 71), 0),
        "bottleneck": scatter_about(key_list[1], (CLIPS, NB, D), 1.0, 6.0, ((0, 16),)),
        "clip_ids": draw_clip_ids(jax.random.fold_in(key_list[12], 71), 0),
        "expert_ids": draw_expert_ids(jax.random.fold_in(key_list[12], 71), 0),
        "slots": draw_slots(jax.random.fold_in(key_list[12], 71), 0),
        "norm1_gain": jnp.clip(1.0 + 0.18 * jax.random.normal(key_list[5], (2, D), jnp.float32), 0.099609375, 1.8984375).astype(jnp.bfloat16),
        "attn_qkv": draw_attn_qkv(jax.random.fold_in(key_list[12], 71), 0),
        "attn_out": scatter_about(key_list[7], (2, D, D), D ** -0.5, 0.1875, ((0, 2),)),
        "norm2_gain": jnp.clip(1.0 + 0.18 * jax.random.normal(key_list[8], (2, D), jnp.float32), 0.099609375, 1.8984375).astype(jnp.bfloat16),
        "router": scatter_about(key_list[9], (D, EXPERTS), D ** -0.5, 0.1875),
        "fc_in": scatter_about(key_list[10], (EXPERTS, D, FF), D ** -0.5, 0.1875, ((0, 16),)),
        "fc_out": scatter_about(key_list[11], (EXPERTS, FF, D), FF ** -0.5, 0.09375, ((0, 16),)),
    }


EPSILON = 1e-06

def layer_norm(features, scales):
    row_mean = lax.optimization_barrier(jnp.mean(features, axis=-1, keepdims=True))
    centred = features - row_mean
    spread = lax.optimization_barrier(jnp.mean(centred * centred, axis=-1, keepdims=True))
    return centred * lax.rsqrt(spread + EPSILON) * scales.astype(jnp.float32)

def attend(token_rows, latent_rows, token_clip, clip_start, scales, w_qkv, w_out):
    n_clips, n_latent, model_width = latent_rows.shape
    n_tokens = token_rows.shape[0]
    all_rows = jnp.concatenate([token_rows, latent_rows.reshape(n_clips * n_latent, model_width)], axis=0)
    row_count = all_rows.shape[0]
    head_count = model_width // HEAD
    normed = layer_norm(all_rows.astype(jnp.float32), scales).astype(jnp.bfloat16)
    packed = jnp.dot(normed, w_qkv, preferred_element_type=jnp.float32).astype(jnp.bfloat16)
    queries = packed[:, :model_width].reshape(row_count, head_count, HEAD)
    key_rows = packed[:, model_width:2 * model_width].reshape(row_count, head_count, HEAD)
    value_rows = packed[:, 2 * model_width:].reshape(row_count, head_count, HEAD)
    latent_clip = clip_start + jnp.arange(n_clips * n_latent, dtype=jnp.int32) // n_latent
    row_clip = jnp.concatenate([token_clip.astype(jnp.int32), latent_clip.astype(jnp.int32)])
    allowed = row_clip[:, None] == row_clip[None, :]
    scores = jnp.einsum('qhd,khd->hqk', queries.astype(jnp.float32), key_rows.astype(jnp.float32)) * (1.0 / math.sqrt(HEAD))
    scores = jnp.where(allowed[None, :, :], scores, -jnp.inf)
    row_max = lax.optimization_barrier(jnp.max(scores, axis=-1, keepdims=True))
    weights = jnp.exp(scores - row_max)
    attn_weights = (weights / lax.optimization_barrier(jnp.sum(weights, axis=-1, keepdims=True))).astype(jnp.bfloat16)
    attended = jnp.einsum('hqk,khd->qhd', attn_weights.astype(jnp.float32), value_rows.astype(jnp.float32))
    attended = attended.reshape(row_count, model_width).astype(jnp.bfloat16)
    updated = all_rows.astype(jnp.float32) + jnp.dot(attended, w_out, preferred_element_type=jnp.float32)
    return (updated[:n_tokens], updated[n_tokens:].reshape(n_clips, n_latent, model_width))

def expert_step(operands):
    block_rows, weight_in, weight_out = operands
    hidden_units = jnp.dot(block_rows, weight_in, preferred_element_type=jnp.float32)
    activated = jax.nn.gelu(hidden_units, approximate=False).astype(jnp.bfloat16)
    return jnp.dot(activated, weight_out, preferred_element_type=jnp.float32).astype(jnp.bfloat16)

def reference(tokens, bottleneck, clip_ids, expert_ids, slots, norm1_gain, attn_qkv, attn_out, norm2_gain, router, fc_in, fc_out):
    model_width = tokens.shape[-1]
    blocks = tokens.shape[1] // TOK_DEV
    latent = bottleneck.reshape(blocks, CLIPS_DEV, NB, model_width)
    starts = jnp.arange(blocks, dtype=jnp.int32) * CLIPS_DEV
    block_of = jnp.arange(blocks * TOK_DEV, dtype=jnp.int32) // TOK_DEV
    column = jnp.arange(EXPERTS, dtype=jnp.int32)
    slot_total = EXPERTS * blocks * CAP
    outputs = []
    latents = []
    for modality in range(2):

        def one_block(operands):
            token_rows, latent_rows, token_clip, clip_start = operands
            return attend(token_rows, latent_rows, token_clip, clip_start, norm1_gain[modality], attn_qkv[modality], attn_out[modality])
        mid_tokens, mid_latent = lax.map(one_block, (tokens[modality].reshape(blocks, TOK_DEV, model_width), latent, clip_ids[modality].reshape(blocks, TOK_DEV), starts))
        mid_tokens = mid_tokens.reshape(blocks * TOK_DEV, model_width)
        latents.append(mid_latent)
        expert_in = layer_norm(mid_tokens, norm2_gain[modality]).astype(jnp.bfloat16)
        logits = jnp.dot(expert_in, router, preferred_element_type=jnp.float32)
        chosen = expert_ids[modality].astype(jnp.int32)
        slot_ids = slots[modality].astype(jnp.int32)
        picked = lax.optimization_barrier(jnp.sum(jnp.where(column[None, :] == chosen[:, None], logits, jnp.zeros_like(logits)), axis=1))
        gate_value = jax.nn.sigmoid(picked)
        served = slot_ids < CAP
        position = jnp.where(served, chosen * (blocks * CAP) + block_of * CAP + slot_ids, slot_total).astype(jnp.int32)
        buffer = jnp.zeros((slot_total, model_width), jnp.bfloat16).at[position].set(expert_in, mode='drop')
        served_rows = lax.map(expert_step, (buffer.reshape(EXPERTS, blocks * CAP, model_width), fc_in, fc_out))
        served_rows = served_rows.reshape(slot_total, model_width)
        returned = jnp.take(served_rows, position, axis=0, mode='fill', fill_value=0)
        outputs.append((mid_tokens + gate_value[:, None] * returned.astype(jnp.float32)).astype(jnp.bfloat16))
    mixed_tokens = jnp.stack(outputs)
    new_bottleneck = ((latents[0] + latents[1]) * 0.5).astype(jnp.bfloat16).reshape(blocks * CLIPS_DEV, NB, model_width)
    return (mixed_tokens, new_bottleneck)
```

```python
import functools
import math

import jax
import jax.numpy as jnp
from jax import lax
from jax.experimental import pallas as pl
from jax.experimental.pallas import tpu as pltpu
from jax.sharding import PartitionSpec as P

HEAD = 64
CAP_FACTOR = 2
EPSILON = 1e-06
STEP_HEADS = 4
LOG2E = math.log2(math.e)


def layer_norm(features, scales):
    row_mean = jnp.mean(features, axis=-1, keepdims=True)
    centred = features - row_mean
    spread = jnp.mean(centred * centred, axis=-1, keepdims=True)
    return centred * lax.rsqrt(spread + EPSILON) * scales.astype(jnp.float32)


def attention_kernel(
    tokens_ref,
    latent_ref,
    clip_col_ref,
    clip_row_ref,
    gain1_ref,
    wq_ref,
    wk_ref,
    wv_ref,
    wo_ref,
    gain2_ref,
    router_ref,
    chosen_ref,
    position_ref,
    mid_ref,
    gate_ref,
    latent_out_ref,
    *rest,
    n_tokens,
    capacity,
    steps,
):
    send_refs = rest[:-4]
    normed_ref, bias_ref, acc_ref, expert_in_ref = rest[-4:]
    step = pl.program_id(0)
    rows = acc_ref.shape[0]
    width = STEP_HEADS * HEAD

    @pl.when(step == 0)
    def _():
        tok = tokens_ref[...].astype(jnp.float32)
        lat = latent_ref[...].astype(jnp.float32)
        acc_ref[:n_tokens, :] = tok
        acc_ref[n_tokens:, :] = lat
        normed_ref[:n_tokens, :] = layer_norm(tok, gain1_ref[...]).astype(jnp.bfloat16)
        normed_ref[n_tokens:, :] = layer_norm(lat, gain1_ref[...]).astype(jnp.bfloat16)
        bias_ref[...] = jnp.where(clip_col_ref[...] == clip_row_ref[...], 0.0, -jnp.inf)

    normed = normed_ref[...]
    scale = 1.0 / math.sqrt(HEAD)
    q = jnp.dot(normed, wq_ref[...], preferred_element_type=jnp.float32).astype(jnp.bfloat16)
    k = jnp.dot(normed, wk_ref[...], preferred_element_type=jnp.float32).astype(jnp.bfloat16)
    v = jnp.dot(normed, wv_ref[...], preferred_element_type=jnp.float32).astype(jnp.bfloat16)
    lane_head = lax.broadcasted_iota(jnp.int32, (1, width), 1) // HEAD
    att = jnp.zeros((rows, width), jnp.float32)
    for h in range(STEP_HEADS):
        mine = lane_head == h
        kh = jnp.where(mine, k, jnp.zeros_like(k))
        s = lax.dot_general(
            q, kh, (((1,), (1,)), ((), ())), preferred_element_type=jnp.float32
        )
        s = s * (scale * LOG2E) + bias_ref[...]
        w = jnp.exp2(s - jnp.max(s, axis=-1, keepdims=True)).astype(jnp.bfloat16)
        vh = jnp.where(mine, v, jnp.ones_like(v))
        o = jnp.dot(w, vh, preferred_element_type=jnp.float32)
        lane = ((h + 2) % STEP_HEADS) * HEAD
        total = o[:, lane : lane + 1]
        att = jnp.where(mine, o * (1.0 / total), att)
    acc_ref[...] += jnp.dot(
        att.astype(jnp.bfloat16), wo_ref[...], preferred_element_type=jnp.float32
    )

    @pl.when(step == steps - 1)
    def _():
        mid = acc_ref[:n_tokens, :]
        mid_ref[...] = mid
        latent_out_ref[...] = acc_ref[n_tokens:, :].astype(jnp.bfloat16)
        expert_in = layer_norm(mid, gain2_ref[...]).astype(jnp.bfloat16)
        expert_in_ref[...] = expert_in
        logits = jnp.dot(expert_in, router_ref[...], preferred_element_type=jnp.float32)
        column = lax.broadcasted_iota(jnp.int32, logits.shape, 1)
        picked = jnp.sum(
            jnp.where(column == chosen_ref[...], logits, 0.0), axis=1, keepdims=True
        )
        gate_ref[...] = jax.nn.sigmoid(picked)
        together = max(1, 256 // capacity)
        for first in range(0, len(send_refs), together):
            part = send_refs[first : first + together]
            slot = first * capacity + lax.broadcasted_iota(
                jnp.int32, (len(part) * capacity, n_tokens), 0
            )
            pick = jnp.where(slot == position_ref[...], 1.0, 0.0).astype(jnp.bfloat16)
            block = jnp.dot(
                pick, expert_in_ref[...], preferred_element_type=jnp.float32
            ).astype(jnp.bfloat16)
            for i, ref in enumerate(part):
                ref[...] = block[i * capacity : (i + 1) * capacity]


def attend_and_dispatch(
    tokens, latent, clip_col, clip_row, gain1, w_qkv, w_out, gain2, router, chosen, position,
    expert_count, capacity,
):
    n_tokens, model_width = tokens.shape
    n_latent = latent.shape[0]
    rows = n_tokens + n_latent
    width = STEP_HEADS * HEAD
    steps = model_width // width
    whole = lambda a: pl.BlockSpec(a.shape, lambda g: (0,) * a.ndim)
    full = lambda shape: pl.BlockSpec(shape, lambda g: (0, 0))
    out_shapes = [
        jax.ShapeDtypeStruct((n_tokens, model_width), jnp.float32),
        jax.ShapeDtypeStruct((n_tokens, 1), jnp.float32),
        jax.ShapeDtypeStruct((n_latent, model_width), jnp.bfloat16),
    ] + [jax.ShapeDtypeStruct((capacity, model_width), jnp.bfloat16)] * expert_count
    return pl.pallas_call(
        functools.partial(
            attention_kernel, n_tokens=n_tokens, capacity=capacity, steps=steps
        ),
        grid=(steps,),
        in_specs=[
            whole(tokens),
            whole(latent),
            whole(clip_col),
            whole(clip_row),
            whole(gain1),
            pl.BlockSpec((model_width, width), lambda g: (0, g)),
            pl.BlockSpec((model_width, width), lambda g: (0, steps + g)),
            pl.BlockSpec((model_width, width), lambda g: (0, 2 * steps + g)),
            pl.BlockSpec((width, model_width), lambda g: (g, 0)),
            whole(gain2),
            whole(router),
            whole(chosen),
            whole(position),
        ],
        out_specs=[full(s.shape) for s in out_shapes],
        out_shape=out_shapes,
        scratch_shapes=[
            pltpu.VMEM((rows, model_width), jnp.bfloat16),
            pltpu.VMEM((rows, rows), jnp.float32),
            pltpu.VMEM((rows, model_width), jnp.float32),
            pltpu.VMEM((n_tokens, model_width), jnp.bfloat16),
        ],
        compiler_params=pltpu.CompilerParams(
            dimension_semantics=("arbitrary",), vmem_limit_bytes=52 << 20
        ),
        cost_estimate=pl.CostEstimate(
            flops=12_000_000_000, bytes_accessed=12 << 20, transcendentals=5_000_000
        ),
        name="attend",
    )(
        tokens, latent, clip_col, clip_row, gain1, w_qkv, w_qkv, w_qkv, w_out, gain2, router,
        chosen, position,
    )


def gelu(x):
    return 0.5 * x * (1.0 + lax.erf(x * math.sqrt(0.5)))


def expert_kernel(*refs, count, steps):
    in_refs = refs[:count]
    w_in_ref, w_out_ref = refs[count : count + 2]
    out_refs = refs[count + 2 : 2 * count + 2]
    rows_ref, acc_ref = refs[2 * count + 2 :]
    capacity = in_refs[0].shape[0]
    total = rows_ref.shape[0]
    step = pl.program_id(0)

    @pl.when(step == 0)
    def _():
        for i in range(count):
            rows_ref[i * capacity : (i + 1) * capacity, :] = in_refs[i][...]
        acc_ref[...] = jnp.zeros_like(acc_ref)

    piece = min(total, 256)
    for first in range(0, total, piece):
        hidden = jnp.dot(
            rows_ref[first : first + piece, :], w_in_ref[0], preferred_element_type=jnp.float32
        )
        hidden = gelu(hidden).astype(jnp.bfloat16)
        acc_ref[first : first + piece, :] += jnp.dot(
            hidden, w_out_ref[0], preferred_element_type=jnp.float32
        )

    @pl.when(step == steps - 1)
    def _():
        for i in range(count):
            out_refs[i][...] = acc_ref[i * capacity : (i + 1) * capacity, :].astype(jnp.bfloat16)


def run_expert(blocks, fc_in, fc_out, name):
    count = len(blocks)
    capacity, model_width = blocks[0].shape
    hidden_width = fc_in.shape[2]
    chunk = min(hidden_width, 512)
    steps = hidden_width // chunk
    total = count * capacity
    spec = pl.BlockSpec((capacity, model_width), lambda g: (0, 0))
    return pl.pallas_call(
        functools.partial(expert_kernel, count=count, steps=steps),
        grid=(steps,),
        in_specs=[spec] * count
        + [
            pl.BlockSpec((1, model_width, chunk), lambda g: (0, 0, g)),
            pl.BlockSpec((1, chunk, model_width), lambda g: (0, g, 0)),
        ],
        out_specs=[spec] * count,
        out_shape=[jax.ShapeDtypeStruct((capacity, model_width), jnp.bfloat16)] * count,
        scratch_shapes=[
            pltpu.VMEM((total, model_width), jnp.bfloat16),
            pltpu.VMEM((total, model_width), jnp.float32),
        ],
        compiler_params=pltpu.CompilerParams(
            dimension_semantics=("arbitrary",), vmem_limit_bytes=40 << 20
        ),
        cost_estimate=pl.CostEstimate(
            flops=4 * total * model_width * hidden_width,
            bytes_accessed=4 * model_width * hidden_width,
            transcendentals=total * hidden_width,
        ),
        name=name,
    )(*blocks, fc_in, fc_out)


def combine_kernel(*refs, count):
    back_refs = refs[:count]
    mid_ref, gate_ref, position_ref, out_ref = refs[count:]
    capacity = back_refs[0].shape[0]
    n_tokens = mid_ref.shape[0]
    together = max(1, 256 // capacity)
    returned = None
    for first in range(0, count, together):
        part = back_refs[first : first + together]
        slot = first * capacity + lax.broadcasted_iota(
            jnp.int32, (n_tokens, len(part) * capacity), 1
        )
        pick = jnp.where(slot == position_ref[...], 1.0, 0.0).astype(jnp.bfloat16)
        values = jnp.concatenate([r[...] for r in part], axis=0)
        product = jnp.dot(pick, values, preferred_element_type=jnp.float32)
        returned = product if returned is None else returned + product
    out_ref[...] = (mid_ref[...] + gate_ref[...] * returned).astype(jnp.bfloat16)


def combine(blocks, mid, gate, position):
    return pl.pallas_call(
        functools.partial(combine_kernel, count=len(blocks)),
        out_shape=jax.ShapeDtypeStruct(mid.shape, jnp.bfloat16),
        compiler_params=pltpu.CompilerParams(vmem_limit_bytes=40 << 20),
        cost_estimate=pl.CostEstimate(
            flops=2_000_000_000, bytes_accessed=5 << 20, transcendentals=0
        ),
        name="combine",
    )(*blocks, mid, gate, position)


def on_device(
    experts_axis,
    tokens,
    bottleneck,
    clip_ids,
    expert_ids,
    slots,
    norm1_gain,
    attn_qkv,
    attn_out,
    norm2_gain,
    router,
    fc_in,
    fc_out,
):
    n_clips, n_latent, model_width = bottleneck.shape
    n_tokens = tokens.shape[1]
    expert_count = router.shape[1]
    capacity = CAP_FACTOR * n_tokens // expert_count
    me = lax.axis_index("exp")
    clip_start = me * n_clips
    latent_clip = clip_start + jnp.arange(n_clips * n_latent, dtype=jnp.int32) // n_latent
    row_clip = jnp.concatenate([clip_ids[0], latent_clip])
    served = slots[0] < capacity
    position = jnp.where(served, (expert_ids[0] ^ me) * capacity + slots[0], -1)
    mid, gate, mid_latent, *blocks = attend_and_dispatch(
        tokens[0],
        bottleneck.reshape(n_clips * n_latent, model_width),
        row_clip[:, None],
        row_clip[None, :],
        norm1_gain,
        attn_qkv[0],
        attn_out[0],
        norm2_gain,
        router,
        expert_ids[0][:, None],
        position[None, :],
        expert_count,
        capacity,
    )

    def exchange(block, s):
        pairs = [(i, i ^ s) for i in range(experts_axis)]
        return lax.ppermute(block, "exp", pairs)

    half, quarter = experts_axis // 2, experts_axis // 4
    groups = [
        ("far_a", range(half, half + quarter)),
        ("near", range(0, half)),
        ("far_b", range(half + quarter, experts_axis)),
    ]
    arrived = {0: blocks[0]}
    for _, members in groups:
        for s in members:
            if s:
                arrived[s] = exchange(blocks[s], s)
    other = lax.ppermute(mid_latent, "mod", [(0, 1), (1, 0)])
    returned = {}
    for name, members in groups:
        results = run_expert([arrived[s] for s in members], fc_in, fc_out, name)
        for s, block in zip(members, results):
            returned[s] = exchange(block, s) if s else block
    new_bottleneck = (
        (mid_latent.astype(jnp.float32) + other.astype(jnp.float32)) * 0.5
    ).astype(jnp.bfloat16)
    mixed = combine(
        [returned[s] for s in range(experts_axis)], mid, gate, position[:, None]
    )
    return (mixed[None], new_bottleneck.reshape(bottleneck.shape))


def solution(mesh):
    in_specs = (
        P("mod", "exp", None),
        P("exp", None, None),
        P("mod", "exp"),
        P("mod", "exp"),
        P("mod", "exp"),
        P("mod", None),
        P("mod", None, None),
        P("mod", None, None),
        P("mod", None),
        P(),
        P("exp", None, None),
        P("exp", None, None),
    )
    out_specs = (P("mod", "exp", None), P("exp", None, None))
    return jax.shard_map(
        functools.partial(on_device, mesh.shape["exp"]),
        mesh=mesh,
        in_specs=in_specs,
        out_specs=out_specs,
        check_vma=False,
    )
```
